32 devices in a mesh: cfg: 2 (over y), ta: 4 (over z), xyz: 4 (over x, core).
Axes of the slice: x: 2, y: 2, z: 4, core: 2. Of those that a mesh axis runs over, the one named last changes fastest.
Arguments:
- sink: float32 [24, 4, 3, 2, 4, 32, 128], P('cfg', None, None, None, 'ta', 'xyz'), parts along dimension 0, may hold values from -6 to 6
- links: float32 [16, 4, 3, 3, 2, 4, 32, 128], P('cfg', None, None, None, None, 'ta', 'xyz'), parts along dimension 0, may hold values from -2 to 2
- section_index: int32 [2, 3], replicated, may hold values from 0 to 7
- momenta: int32 [33, 3], replicated, may hold values from -3 to 3
- source: int32 [3], replicated, may hold values from 0 to 15
Outputs:
- adjoint: float32 [24, 4, 3, 2, 4, 32, 128], P('cfg', None, None, None, 'ta', 'xyz'), parts along dimension 0
- correlator: float32 [4, 33, 4], P('cfg', None, 'ta'), parts along dimension 0
The draws below stay inside these ranges and needn't reach their ends.
There are 2 independent parts, one for each index of `cfg`. The reference program is written for one: setup_inputs(seed, part) draws one part's arguments, and reference() takes and returns one part's arrays. A program takes and returns all parts, laid end to end along the dimension named above; an argument that names none is the same for every part. Nothing has to cross between parts.
All inputs are finite; a program needn't handle non-finite values.
Results may differ from the reference program's by a relative error of at most 0.000068.
Values sent between devices are 32-bit elements; how exact they have to be, the bound alone decides.
A program may use at most 128 MiB of HBM per device.

```python
import math
import jax
import jax.numpy as jnp
from jax import lax

NCOL = 12
NMOM = 33
STEPS = 2
SLOTS = 8
LY = 16
NT = 4
NX = 32
NY = 16
NZ = 8


def touch_ends(drawn, rng, least, largest):
    dims = drawn.shape
    index_at = [jax.random.randint(jax.random.fold_in(rng, axis), (), 0, dims[axis]) for axis in range(len(dims))]
    drawn = drawn.at[tuple(index_at)].set(least)
    longest = dims.index(max(dims))
    index_at[longest] = (index_at[longest] + 1) % dims[longest]
    return drawn.at[tuple(index_at)].set(largest)


def block_scale(stream_key, shape, cuts, smallest, high):
    loudness = 1.0
    for position, blocks in cuts:
        draws = jax.random.uniform(jax.random.fold_in(jax.random.fold_in(stream_key, 6), position), (blocks,), jnp.float32, smallest / len(cuts), high / len(cuts))
        loudness = loudness * jnp.repeat(jnp.exp(draws), shape[position] // blocks).reshape((-1,) + (1,) * (len(shape) - 1 - position))
    return loudness


def bell_draw(rng, dims, spread, reach, pieces=(), held_as=jnp.bfloat16):
    result = jax.random.normal(rng, dims, jnp.float32) * spread
    if len(pieces) > 0:
        result = block_scale(rng, dims, pieces, -0.22, 0.18) * result
    return jnp.clip(result, min=-reach, max=reach).astype(held_as)


def setup_inputs(seed: int = 0, part: int = 0) -> dict:
    seeds = jax.random.split(jax.random.key(seed), 6)
    own_keys = jax.random.split(jax.random.fold_in(seeds[5], part), 6)
    return {
        "sink": bell_draw(own_keys[0], (NCOL, 4, 3, 2, NT, NX, NY * NZ), 1.0, 6.0, ((4, 4), (5, 4)), jnp.float32),
        "links": bell_draw(own_keys[1], (SLOTS, 4, 3, 3, 2, NT, NX, NY * NZ), 0.35, 2.0, ((5, 4), (6, 4)), jnp.float32),
        "section_index": touch_ends(jax.random.randint(seeds[2], (STEPS, 3), 0, SLOTS), jax.random.fold_in(seeds[2], 1), 0, SLOTS - 1).astype(jnp.int32),
        "momenta": touch_ends(jax.random.randint(seeds[3], (NMOM, 3), -3, 4), jax.random.fold_in(seeds[3], 1), -3, 3).astype(jnp.int32),
        "source": jax.random.randint(seeds[4], (3,), 0, LY).astype(jnp.int32),
    }


flow_step = 0.05

def hop_forward(matrix, field):
    spin_real = field[:, :, :, 0]
    spin_imag = field[:, :, :, 1]
    terms_real = []
    terms_imag = []
    for colour in range(3):
        link_real = matrix[:, colour, 0][None, None]
        link_imag = matrix[:, colour, 1][None, None]
        part_real = spin_real[:, :, colour][:, :, None]
        part_imag = spin_imag[:, :, colour][:, :, None]
        terms_real.append(link_real * part_real - link_imag * part_imag)
        terms_imag.append(link_real * part_imag + link_imag * part_real)
    return jnp.stack([terms_real[0] + terms_real[1] + terms_real[2], terms_imag[0] + terms_imag[1] + terms_imag[2]], axis=3)

def hop_backward(matrix, field):
    spin_real = field[:, :, :, 0]
    spin_imag = field[:, :, :, 1]
    terms_real = []
    terms_imag = []
    for colour in range(3):
        link_real = matrix[colour, :, 0][None, None]
        link_imag = matrix[colour, :, 1][None, None]
        part_real = spin_real[:, :, colour][:, :, None]
        part_imag = spin_imag[:, :, colour][:, :, None]
        terms_real.append(link_real * part_real + link_imag * part_imag)
        terms_imag.append(link_real * part_imag - link_imag * part_real)
    return jnp.stack([terms_real[0] + terms_real[1] + terms_real[2], terms_imag[0] + terms_imag[1] + terms_imag[2]], axis=3)

def shift_inner(field, amount):
    zcoord = jnp.arange(NY * NZ, dtype=jnp.int32) % NZ
    if amount < 0:
        inside = jnp.roll(field, -1, axis=-1)
        wrapped = jnp.roll(field, NZ - 1, axis=-1)
        return jnp.where(zcoord == NZ - 1, wrapped, inside)
    inside = jnp.roll(field, 1, axis=-1)
    wrapped = jnp.roll(field, 1 - NZ, axis=-1)
    return jnp.where(zcoord == 0, wrapped, inside)

def roll_lattice(field, direction, amount):
    if direction == 0:
        return jnp.roll(field, amount, axis=-3)
    if direction == 1:
        return jnp.roll(field, amount, axis=-2)
    if direction == 2:
        return jnp.roll(field, amount * NZ, axis=-1)
    return shift_inner(field, amount)

def laplacian(field, section_links):
    total = -8.0 * field
    for direction in range(4):
        matrix = section_links[direction]
        total = total + hop_forward(matrix, roll_lattice(field, direction, -1))
        total = total + roll_lattice(hop_backward(matrix, field), direction, 1)
    return total

def adjoint_step(lam, first, second, third):
    coef_third = 0.75 * flow_step
    coef_second = 8.0 * flow_step / 9.0
    coef_first = 0.25 * flow_step
    coef_mixed = 2.0 * flow_step / 9.0
    later = coef_third * laplacian(lam, third)
    middle = lam + coef_second * laplacian(later, second)
    return middle + later + laplacian(coef_first * middle - coef_mixed * later, first)

def phase_table(xcoord, nx_total, momenta, source):
    plane_index = jnp.arange(NY * NZ, dtype=jnp.int32)
    ycoord = plane_index // NZ
    zcoord = plane_index % NZ
    dist_x = jnp.mod(xcoord - source[0], nx_total)
    dist_y = jnp.mod(ycoord - source[1], NY)
    dist_z = jnp.mod(zcoord - source[2], NZ)
    frac_x = jnp.mod(momenta[:, 0:1] * dist_x[None, :], nx_total).astype(jnp.float32) / float(nx_total)
    frac_y = jnp.mod(momenta[:, 1:2] * dist_y[None, :], NY).astype(jnp.float32) / float(NY)
    frac_z = jnp.mod(momenta[:, 2:3] * dist_z[None, :], NZ).astype(jnp.float32) / float(NZ)
    frac = frac_x[:, :, None] + frac_y[:, None, :] + frac_z[:, None, :]
    angle = 2.0 * math.pi * frac
    table = jnp.concatenate([jnp.cos(angle), -jnp.sin(angle)], axis=0)
    return table.reshape(2 * NMOM, xcoord.shape[0] * NY * NZ)

def reference(sink, links, section_index, momenta, source):
    lam = sink
    for step in reversed(range(STEPS)):
        sections = [lax.dynamic_index_in_dim(links, section_index[step, section], 0, keepdims=False) for section in range(3)]
        lam = adjoint_step(lam, sections[0], sections[1], sections[2])
    squares = lax.optimization_barrier(jnp.sum(lam * lam, axis=(0, 2, 3)))
    density = squares[0] + squares[1] - squares[2] - squares[3]
    density = density.reshape(NT, NX * NY * NZ)
    table = phase_table(jnp.arange(NX, dtype=jnp.int32), NX, momenta, source)
    projected = jnp.dot(density, table.T, precision=lax.Precision.HIGHEST)
    scale = 1.0 / math.sqrt(576.0 * NX * NY * NZ)
    projected = projected * scale
    correlator = jnp.transpose(projected.reshape(NT, 2, NMOM), (1, 2, 0))
    return (lam, correlator)
```

```python
import functools
import math

import jax
import jax.numpy as jnp
from jax import lax
from jax.experimental import pallas as pl
from jax.experimental.pallas import tpu as pltpu
from jax.sharding import PartitionSpec as P

STEPS = 2
NY = 16
NZ = 8
SECTIONS = 3 * STEPS
MESH = pl.DeviceIdType.MESH

flow_step = 0.05


def remote(src, dst, send_sem, recv_sem, axis, peer):
    return pltpu.make_async_remote_copy(
        src_ref=src, dst_ref=dst, send_sem=send_sem, recv_sem=recv_sem,
        device_id={axis: peer}, device_id_type=MESH,
    )


def roll3(x, amount, axis):
    shape = x.shape
    flat = x.reshape((-1,) + shape[-2:])
    return pltpu.roll(flat, amount % flat.shape[axis], axis).reshape(shape)


def hop(acc, link, x, conj):
    one, two, three = acc
    for k in range(3):
        vr, vi = x[2 * k], x[2 * k + 1]
        vs = (vr + vi)[None]
        if conj:
            block = link[k]
            a, b, c = block[:, 0] * vs, block[:, 2] * vi[None], block[:, 1] * vr[None]
            two = -b if two is None else two - b
            three = -c if three is None else three - c
        else:
            block = link[:, k]
            a, b, c = block[:, 0] * vs, block[:, 1] * vi[None], block[:, 2] * vr[None]
            two = b if two is None else two + b
            three = c if three is None else three + c
        one = a if one is None else one + a
    return one, two, three


def kernel(n, nx, nc, lo, hi, parts, nmom, order_ref, source_ref, momenta_ref, sink_ref, link_ref,
           out_ref, proj_ref,
           raw, lk, cur, lam, later, mixed, hs, hr, rs, rr, table, dens, pjs, pjr, pjt, pjf,
           raw_sem, loc_sem, fs_sem, fr_sem, ls_sem, lr_sem,
           hss_sem, hsr_sem, rs_sem, rr_sem, os_sem, or_sem, oloc_sem,
           xs_sem, xr_sem, ts_sem, tr_sem):
    me = lax.axis_index("ta")
    mx = lax.axis_index("xyz")
    worker = jnp.logical_and(me >= lo, me < hi)
    mine = me - lo
    workers = hi - lo
    share = nc // parts
    slots = raw.shape[0]
    cells = 8
    left, right = lax.rem(mx + nx - 1, nx), lax.rem(mx + 1, nx)
    sub = lax.broadcasted_iota(jnp.int32, (8, 128), 0)
    zc = lax.broadcasted_iota(jnp.int32, (8, 128), 1) % NZ

    for slot in range(slots):
        pltpu.make_async_copy(link_ref.at[slot], raw.at[slot], raw_sem.at[slot]).start()

    def own_copy(part):
        return pltpu.make_async_copy(sink_ref.at[pl.ds(mine * nc + part * share, share)],
                                     lam.at[me, pl.ds(part * share, share)], loc_sem.at[part])

    @pl.when(worker)
    def _():
        for part in range(parts):
            own_copy(part).start()

    barrier = pltpu.get_barrier_semaphore()
    for d in range(1, n):
        pl.semaphore_signal(barrier, inc=1, device_id={"ta": lax.rem(me + d, n)}, device_id_type=MESH)
    for d in range(1, nx):
        pl.semaphore_signal(barrier, inc=1, device_id={"xyz": lax.rem(mx + d, nx)}, device_id_type=MESH)
    pl.semaphore_wait(barrier, n + nx - 2)

    def field_copy(j, source, part):
        return remote(sink_ref.at[pl.ds(j * nc + part * share, share)],
                      lam.at[source, pl.ds(part * share, share)],
                      fs_sem.at[j, part], fr_sem.at[source, part], "ta", lo + j)

    def link_copy(s, j, source):
        return remote(lk.at[s, source], lk.at[s, source], ls_sem.at[s, j], lr_sem.at[s, source], "ta", lo + j)

    def peer_order(i):
        return jnp.where(me < n // 2, workers - 1 - i, i)

    def to_workers(act):
        for i in range(workers):
            j = peer_order(i)

            @pl.when(me != lo + j)
            def _():
                act(j)

    for part in range(parts):
        to_workers(lambda j: field_copy(j, me, part).start())

    for slot in range(slots):
        pltpu.make_async_copy(link_ref.at[slot], raw.at[slot], raw_sem.at[slot]).wait()

    for s in range(SECTIONS):
        slot = order_ref[STEPS - 1 - s // 3, 2 - s % 3]
        for g in range(4):
            lk[s, me, g * 18:(g + 1) * 18] = raw[slot, g * 18:(g + 1) * 18]
        to_workers(lambda j: link_copy(s, j, me).start())

    def fill_table():
        nx_total = cells * nx
        lane = lax.broadcasted_iota(jnp.int32, (8, 128), 1)
        table[0, 0:8] = jnp.zeros((8, 128), jnp.float32)
        table[0, 0:3, 0:nmom] = momenta_ref[...].astype(jnp.float32)
        base = table[0, 0:8]
        both = jnp.where(lane < 64, base, pltpu.roll(base, 64, 1))
        quarter = jnp.where(lane < 64, 0.0, 0.25)
        shape = (NY * NZ, 128)
        site = lax.broadcasted_iota(jnp.int32, shape, 0)
        yd = (site // NZ - source_ref[1]).astype(jnp.float32)
        zd = (site % NZ - source_ref[2]).astype(jnp.float32)

        def part_of(p, d, size):
            f = (p * d) * (1.0 / size)
            return f - jnp.floor(f)

        base_frac = (part_of(jnp.broadcast_to(both[1:2], shape), yd, NY)
                     + part_of(jnp.broadcast_to(both[2:3], shape), zd, NZ)
                     + jnp.broadcast_to(quarter[0:1], shape))
        px = jnp.broadcast_to(both[0:1], shape)

        for x in range(cells):
            xd = (mx * cells + x - source_ref[0]).astype(jnp.float32)
            frac = base_frac + part_of(px, jnp.full(shape, xd), nx_total)
            frac = frac - jnp.floor(frac + 0.5)
            u = (2.0 * math.pi) * (0.25 - jnp.abs(frac))
            w = u * u
            p = -1.0 / 39916800.0 + w * (1.0 / 6227020800.0)
            for coef in (1.0 / 362880.0, -1.0 / 5040.0, 1.0 / 120.0, -1.0 / 6.0, 1.0):
                p = coef + w * p
            table[x] = u * p

    def halo_copy(s, side, part):
        peer = (left, right)[side]
        return remote(hs.at[s % 2, side, part], hr.at[s % 2, side, part], hss_sem.at[s, side, part],
                      hsr_sem.at[s, side, part], "xyz", peer)

    def put_halo(s, part, t, w, value):
        base = (t * share + w) * 6
        for c in range(6):
            hs[s % 2, 0, part, pl.ds(base + c, 1)] = value[c, 0:1]
            hs[s % 2, 1, part, pl.ds(base + c, 1)] = value[c, 7:8]

    def start_halos(s, part):
        for side in range(2):
            halo_copy(s, side, part).start()

    @pl.when(worker)
    def _():
        fill_table()

        def at_part(part, carry):
            own_copy(part).wait()
            for d in range(1, n):
                field_copy(0, lax.rem(me + d, n), part).wait_recv()

            def first_halo(i, inner):
                t, w = i // share, i % share
                put_halo(0, part, t, w, lam[t, part * share + w])
                return inner

            lax.fori_loop(0, n * share, first_halo, 0)
            start_halos(0, part)
            return carry

        lax.fori_loop(0, parts, at_part, 0)

    def row_copy(s):
        return remote(rs.at[s], rr.at[s], rs_sem.at[s], rr_sem.at[s], "xyz", right)

    def prepare(s):
        def send_rows(t, carry):
            rs[s, t, 0:18] = lk[s, t, 18:36, 7, :]
            return carry

        lax.fori_loop(0, n, send_rows, 0)
        row_copy(s).start()

        def forward(t, carry):
            for d in range(4):
                block = lk[s, t, d * 18:(d + 1) * 18].reshape(9, 2, 8, 128)
                re, im = block[:, 0], block[:, 1]
                cur[t, d] = jnp.stack([re, re + im, im - re], axis=1).reshape(27, 8, 128)
            return carry

        def put_back(t, d, block):
            block = block.reshape(3, 3, 2, 8, 128)
            for a in range(3):
                re, im = block[:, a, 0], block[:, a, 1]
                cur[t, 3 + d, a * 9:(a + 1) * 9] = jnp.stack([re, re - im, -(re + im)], axis=1).reshape(9, 8, 128)

        def backward(t, carry):
            put_back(t, 2, roll3(lk[s, t, 36:54], NZ, 2))
            uz = lk[s, t, 54:72]
            put_back(t, 3, jnp.where((zc == 0)[None], roll3(uz, 1 - NZ, 2), roll3(uz, 1, 2)))
            return carry

        def backward_x(t, carry):
            ux = roll3(lk[s, t, 18:36], 1, 1)
            rows = jnp.broadcast_to(rr[s, t, 0:18][:, None, :], (18, 8, 128))
            put_back(t, 1, jnp.where((sub == 0)[None], rows, ux))
            return carry

        lax.fori_loop(0, n, forward, 0)
        lax.fori_loop(0, n, backward, 0)
        row_copy(s).wait_recv()
        lax.fori_loop(0, n, backward_x, 0)

    def lap(s, part, source, epilogue, after_time):
        par = s % 2

        def at_time(i, carry):
            t = jnp.where(me < n // 2, n - 1 - i, i)
            prev, following = lax.rem(t + n - 1, n), lax.rem(t + 1, n)

            def links(time, d):
                return cur[time, d].reshape(3, 3, 3, 8, 128)

            def at_spinor(w, inner):
                q = part * share + w
                row = (t * share + w) * 6
                v = source[t, q]
                acc = (None, None, None)
                acc = hop(acc, links(t, 0), source[following, q], False)
                acc = hop(acc, links(prev, 0), source[prev, q], True)
                high = jnp.stack([jnp.broadcast_to(hr[par, 0, part, pl.ds(row + c, 1)], (8, 128)) for c in range(6)])
                low = jnp.stack([jnp.broadcast_to(hr[par, 1, part, pl.ds(row + c, 1)], (8, 128)) for c in range(6)])
                acc = hop(acc, links(t, 1), jnp.where((sub == 7)[None], high, roll3(v, -1, 1)), False)
                acc = hop(acc, links(t, 4), jnp.where((sub == 0)[None], low, roll3(v, 1, 1)), False)
                acc = hop(acc, links(t, 2), roll3(v, -NZ, 2), False)
                acc = hop(acc, links(t, 5), roll3(v, NZ, 2), False)
                vf = jnp.where((zc == NZ - 1)[None], roll3(v, NZ - 1, 2), roll3(v, -1, 2))
                acc = hop(acc, links(t, 3), vf, False)
                vb = jnp.where((zc == 0)[None], roll3(v, 1 - NZ, 2), roll3(v, 1, 2))
                acc = hop(acc, links(t, 6), vb, False)
                total = jnp.stack([acc[0] - acc[1], acc[0] + acc[2]], axis=1).reshape(6, 8, 128)
                nxt = epilogue(t, q, total - 8.0 * v, v)
                if nxt is not None:
                    put_halo(s + 1, part, t, w, nxt)
                return inner

            lax.fori_loop(0, share, at_spinor, 0)
            after_time(t, part)
            return carry

        lax.fori_loop(0, n, at_time, 0)

    def ep_later(t, q, value, v):
        value = (0.75 * flow_step) * value
        later[t, q] = value
        return value

    def ep_middle(t, q, value, v):
        middle = lam[t, q] + (8.0 * flow_step / 9.0) * value
        lam[t, q] = middle + v
        value = (0.25 * flow_step) * middle - (2.0 * flow_step / 9.0) * v
        mixed[t, q] = value
        return value

    def ep_last(t, q, value, v):
        value = lam[t, q] + value
        lam[t, q] = value
        square = value * value
        square = (square[0] + square[1]) + (square[2] + square[3]) + (square[4] + square[5])
        sign = jnp.where(lax.rem(q, 4) < 2, 1.0, -1.0)
        dens[t] = dens[t] + sign * square
        return value

    def out_copy(t, part, j):
        return remote(lam.at[t, pl.ds(part * share, share)],
                      out_ref.at[pl.ds(j * nc + part * share, share)],
                      os_sem.at[t, part], or_sem.at[j, part], "ta", t)

    def own_out(part):
        return pltpu.make_async_copy(lam.at[me, pl.ds(part * share, share)],
                                     out_ref.at[pl.ds(mine * nc + part * share, share)], oloc_sem.at[part])

    def nothing(t, part):
        return None

    def step_body(i, carry):
        for k, (source, epilogue) in enumerate(((lam, ep_later), (later, ep_middle), (mixed, ep_last))):
            s = i * 3 + k

            def give(t, part):
                @pl.when(jnp.logical_and(s + 1 == SECTIONS, t != me))
                def _():
                    out_copy(t, part, mine).start()

            for d in range(1, n):
                link_copy(s, 0, lax.rem(me + d, n)).wait_recv()
            prepare(s)
            if k == 2:
                dens[...] = jnp.zeros(dens.shape, jnp.float32)

            def at_part(part, inner):
                for side in range(2):
                    halo_copy(s, side, part).wait()
                lap(s, part, source, epilogue, give if k == 2 else nothing)

                @pl.when(s + 1 < SECTIONS)
                def _():
                    start_halos(s + 1, part)

                @pl.when(s + 1 == SECTIONS)
                def _():
                    own_out(part).start()
                return inner

            lax.fori_loop(0, parts, at_part, 0)
        return carry

    def x_copy(d):
        return remote(pjs, pjr.at[mx], xs_sem.at[d - 1], xr_sem.at[mx], "xyz", lax.rem(mx + d, nx))

    def x_arrival(j):
        return remote(pjs, pjr.at[j], xs_sem.at[0], xr_sem.at[j], "xyz", j)

    def t_copy(t):
        return remote(pjt.at[t], pjf.at[mine], ts_sem.at[t], tr_sem.at[mine], "ta", t)

    @pl.when(worker)
    def _():
        lax.fori_loop(0, STEPS, step_body, 0)
        rows = dens[...].reshape(n * 8, 128)
        cell = lax.broadcasted_iota(jnp.int32, (n * 8, 128), 0) % 8
        acc = jnp.zeros((n * 8, 128), jnp.float32)
        for x in range(cells):
            product = jnp.dot(rows, table[x], precision=lax.Precision.HIGHEST, preferred_element_type=jnp.float32)
            acc = acc + jnp.where(cell == x, product, 0.0)
        pjs[...] = jnp.broadcast_to(jnp.sum(acc.reshape(n, 8, 128), axis=1, keepdims=True), (n, 8, 128))
        pjr[mx] = pjs[...]
        for d in range(1, nx):
            x_copy(d).start()
        for d in range(1, nx):
            x_arrival(lax.rem(mx + d, nx)).wait_recv()
        total = pjr[0]
        for j in range(1, nx):
            total = total + pjr[j]
        pjt[...] = total
        pjf[mine] = pjt[me]
        for d in range(1, n):
            t_copy(lax.rem(me + d, n)).start()

    for j in range(workers):
        @pl.when(me != lo + j)
        def _():
            remote(pjt.at[0], pjf.at[j], ts_sem.at[0], tr_sem.at[j], "ta", lo + j).wait_recv()
    final = pjf[0]
    for j in range(1, workers):
        final = final + pjf[j]
    final = final * (1.0 / math.sqrt(576.0 * cells * nx * NY * NZ))
    proj_ref[0] = final[0:1, 0:nmom]
    proj_ref[1] = pltpu.roll(final, 64, 1)[0:1, 0:nmom]

    def drain(act):
        to_workers(act)

    def drain_parts(part, carry):
        to_workers(lambda j: field_copy(j, me, part).wait_send())
        return carry

    def drain_links(s, carry):
        to_workers(lambda j: link_copy(s, j, me).wait_send())
        return carry

    lax.fori_loop(0, parts, drain_parts, 0)
    lax.fori_loop(0, SECTIONS, drain_links, 0)

    @pl.when(worker)
    def _():
        def drain_rows(s, carry):
            row_copy(s).wait_send()
            return carry

        lax.fori_loop(0, SECTIONS, drain_rows, 0)
        for d in range(1, nx):
            x_copy(d).wait_send()
        for d in range(1, n):
            t_copy(lax.rem(me + d, n)).wait_send()

        def drain_out(part, carry):
            for d in range(1, n):
                out_copy(lax.rem(me + d, n), part, mine).wait_send()
            own_out(part).wait()
            return carry

        lax.fori_loop(0, parts, drain_out, 0)

    def arrivals(part, carry):
        for j in range(workers):
            @pl.when(me != lo + j)
            def _():
                out_copy(lo + j, part, j).wait_recv()
        return carry

    lax.fori_loop(0, parts, arrivals, 0)


def body(n, nx, sink, links, section_index, momenta, source):
    space_cells = sink.shape[5]
    spinors = sink.shape[0] * sink.shape[1]
    slots = links.shape[0]
    nmom = momenta.shape[0]
    lo = n // 4 if spinors % (n - 2 * (n // 4)) == 0 else 0
    hi = n - lo
    nc = spinors // (hi - lo)
    parts = next(p for p in (4, 3, 2, 1) if nc % p == 0)
    share = nc // parts
    workers = hi - lo
    tile = (space_cells, NY * NZ)
    f32 = jnp.float32
    field = pltpu.VMEM((n, nc, 6) + tile, f32)
    halo = pltpu.VMEM((2, 2, parts, n * share * 6, NY * NZ), f32)
    dma = pltpu.SemaphoreType.DMA
    anywhere = pl.BlockSpec(memory_space=pl.ANY)
    vmem = pl.BlockSpec(memory_space=pltpu.VMEM)
    smem = pl.BlockSpec(memory_space=pltpu.SMEM)
    out, proj = pl.pallas_call(
        functools.partial(kernel, n, nx, nc, lo, hi, parts, nmom),
        out_shape=(
            jax.ShapeDtypeStruct((spinors, 6) + tile, f32),
            jax.ShapeDtypeStruct((2, 1, nmom), f32),
        ),
        in_specs=[smem, smem, vmem, anywhere, anywhere],
        out_specs=(anywhere, vmem),
        scratch_shapes=[
            pltpu.VMEM((slots, 72) + tile, f32),
            pltpu.VMEM((SECTIONS, n, 72) + tile, f32),
            pltpu.VMEM((n, 7, 27) + tile, f32),
            field, field, field,
            halo, halo,
            pltpu.VMEM((SECTIONS, n, 24, NY * NZ), f32),
            pltpu.VMEM((SECTIONS, n, 24, NY * NZ), f32),
            pltpu.VMEM((space_cells, NY * NZ, 128), f32),
            pltpu.VMEM((n,) + tile, f32),
            pltpu.VMEM((n, 8, 128), f32),
            pltpu.VMEM((nx, n, 8, 128), f32),
            pltpu.VMEM((n, 8, 128), f32),
            pltpu.VMEM((workers, 8, 128), f32),
            dma((slots,)), dma((parts,)),
            dma((workers, parts)), dma((n, parts)),
            dma((SECTIONS, workers)), dma((SECTIONS, n)),
            dma((SECTIONS, 2, parts)), dma((SECTIONS, 2, parts)),
            dma((SECTIONS,)), dma((SECTIONS,)),
            dma((n, parts)), dma((workers, parts)), dma((parts,)),
            dma((nx - 1,)), dma((nx,)),
            dma((n,)), dma((workers,)),
        ],
        compiler_params=pltpu.CompilerParams(
            collective_id=0, has_side_effects=True, vmem_limit_bytes=63 * 1024 * 1024
        ),
    )(section_index, source, momenta.T, sink.reshape((spinors, 6) + tile), links.reshape((slots, 72) + tile))
    return (out.reshape(sink.shape), jnp.transpose(proj, (0, 2, 1)))


def solution(mesh):
    in_specs = (
        P("cfg", None, None, None, "ta", "xyz", None),
        P("cfg", None, None, None, None, "ta", "xyz", None),
        P(),
        P(),
        P(),
    )
    out_specs = (P("cfg", None, None, None, "ta", "xyz", None), P("cfg", None, "ta"))
    step = functools.partial(body, mesh.shape["ta"], mesh.shape["xyz"])
    return jax.shard_map(step, mesh=mesh, in_specs=in_specs, out_specs=out_specs, check_vma=False)
```

```python
import functools
import math

import jax
import jax.numpy as jnp
from jax import lax
from jax.experimental import pallas as pl
from jax.experimental.pallas import tpu as pltpu
from jax.sharding import PartitionSpec as P

STEPS = 2
NY = 16
NZ = 8
SECTIONS = 3 * STEPS
GROUP = 2
FEWEST = 3
MESH = pl.DeviceIdType.MESH

flow_step = 0.05


def remote(src, dst, send_sem, recv_sem, axis, peer):
    return pltpu.make_async_remote_copy(
        src_ref=src, dst_ref=dst, send_sem=send_sem, recv_sem=recv_sem,
        device_id={axis: peer}, device_id_type=MESH,
    )


def roll3(x, amount, axis):
    shape = x.shape
    flat = x.reshape((-1,) + shape[-2:])
    return pltpu.roll(flat, amount % flat.shape[axis], axis).reshape(shape)


def hop(acc, link, x, conj):
    one, two, three = acc
    for k in range(3):
        vr, vi = x[2 * k], x[2 * k + 1]
        vs = (vr + vi)[None]
        if conj:
            block = link[k]
            a, b, c = block[:, 0] * vs, block[:, 2] * vi[None], block[:, 1] * vr[None]
            two = -b if two is None else two - b
            three = -c if three is None else three - c
        else:
            block = link[:, k]
            a, b, c = block[:, 0] * vs, block[:, 1] * vi[None], block[:, 2] * vr[None]
            two = b if two is None else two + b
            three = c if three is None else three + c
        one = a if one is None else one + a
    return one, two, three


def kernel(n, nx, nc, lo, hi, parts, nmom, distinct, order_ref, source_ref, momenta_ref, sink_ref, link_ref,
           out_ref, proj_ref,
           raw, lk, cur, lam, later, mixed, hs, hr, rs, rr, edge_out, edge_in, table, dens, pjs, pjr, pjt, pjf,
           raw_sem, loc_sem, fs_sem, fr_sem, ls_sem, lr_sem,
           hss_sem, hsr_sem, rs_sem, rr_sem, es_sem, er_sem, gs_sem, gr_sem, os_sem, or_sem,
           xs_sem, xr_sem, ts_sem, tr_sem):
    me = lax.axis_index("ta")
    mx = lax.axis_index("xyz")
    worker = jnp.logical_and(me >= lo, me < hi)
    mine = me - lo
    workers = hi - lo
    share = nc // parts
    group = GROUP if share % GROUP == 0 else 1
    slots = raw.shape[0]
    cells = 8
    left, right = lax.rem(mx + nx - 1, nx), lax.rem(mx + 1, nx)
    sub = lax.broadcasted_iota(jnp.int32, (8, 128), 0)
    zc = lax.broadcasted_iota(jnp.int32, (8, 128), 1) % NZ

    for slot in range(slots):
        pltpu.make_async_copy(link_ref.at[slot], raw.at[slot], raw_sem.at[slot]).start()

    def own_copy(part):
        return pltpu.make_async_copy(sink_ref.at[pl.ds(mine * nc + part * share, share)],
                                     lam.at[me, pl.ds(part * share, share)], loc_sem.at[part])

    @pl.when(worker)
    def _():
        for part in range(parts):
            own_copy(part).start()

    named = [order_ref[STEPS - 1 - s // 3, 2 - s % 3] for s in range(SECTIONS)]
    first, place = [], []
    count = jnp.int32(0)
    for s in range(SECTIONS):
        at = count
        for j in reversed(range(s)):
            at = jnp.where(named[j] == named[s], place[j], at)
        fresh = at == count
        first.append(fresh)
        place.append(at)
        count = count + fresh.astype(jnp.int32)
    held = []
    for d in range(distinct):
        slot = jnp.int32(0)
        for s in range(SECTIONS):
            slot = jnp.where(jnp.logical_and(first[s], place[s] == d), named[s], slot)
        held.append(slot)

    barrier = pltpu.get_barrier_semaphore()
    for d in range(1, n):
        pl.semaphore_signal(barrier, inc=1, device_id={"ta": lax.rem(me + d, n)}, device_id_type=MESH)
    for d in range(1, nx):
        pl.semaphore_signal(barrier, inc=1, device_id={"xyz": lax.rem(mx + d, nx)}, device_id_type=MESH)

    for slot in range(slots):
        pltpu.make_async_copy(link_ref.at[slot], raw.at[slot], raw_sem.at[slot]).wait()
    for d in range(distinct):
        for g in range(4):
            lk[d, me, g * 18:(g + 1) * 18] = raw[held[d], g * 18:(g + 1) * 18]
    edge_out[0:18] = raw[held[distinct - 1], 18:36, 7, :]

    pl.semaphore_wait(barrier, n + nx - 2)

    def field_copy(j, source, part):
        return remote(sink_ref.at[pl.ds(j * nc + part * share, share)],
                      lam.at[source, pl.ds(part * share, share)],
                      fs_sem.at[j, part], fr_sem.at[source, part], "ta", lo + j)

    def link_copy(d, j, source):
        return remote(lk.at[d, source], lk.at[d, source], ls_sem.at[d, j], lr_sem.at[d, source], "ta", lo + j)

    def edge_copy():
        return remote(edge_out, edge_in, es_sem.at[0], er_sem.at[0], "xyz", right)

    def last_rows_copy(j, source):
        return remote(edge_in, rr.at[distinct - 1, source], gs_sem.at[j], gr_sem.at[source], "ta", lo + j)

    def peer_order(i):
        return jnp.where(me < n // 2, workers - 1 - i, i)

    def to_workers(act):
        for i in range(workers):
            j = peer_order(i)

            @pl.when(me != lo + j)
            def _():
                act(j)

    edge_copy().start()
    to_workers(lambda j: link_copy(0, j, me).start())
    for part in range(parts):
        to_workers(lambda j: field_copy(j, me, part).start())
    for d in range(1, distinct - 1):
        to_workers(lambda j: link_copy(d, j, me).start())
    edge_copy().wait_recv()
    to_workers(lambda j: last_rows_copy(j, me).start())
    if distinct > 1:
        to_workers(lambda j: link_copy(distinct - 1, j, me).start())

    @pl.when(worker)
    def _():
        rr[distinct - 1, me] = edge_in[...]

    def fill_table():
        nx_total = cells * nx
        lane = lax.broadcasted_iota(jnp.int32, (8, 128), 1)
        table[0, 0:8] = jnp.zeros((8, 128), jnp.float32)
        table[0, 0:3, 0:nmom] = momenta_ref[...].astype(jnp.float32)
        base = table[0, 0:8]
        both = jnp.where(lane < 64, base, pltpu.roll(base, 64, 1))
        quarter = jnp.where(lane < 64, 0.0, 0.25)
        shape = (NY * NZ, 128)
        site = lax.broadcasted_iota(jnp.int32, shape, 0)
        yd = (site // NZ - source_ref[1]).astype(jnp.float32)
        zd = (site % NZ - source_ref[2]).astype(jnp.float32)

        def part_of(p, d, size):
            f = (p * d) * (1.0 / size)
            return f - jnp.floor(f)

        base_frac = (part_of(jnp.broadcast_to(both[1:2], shape), yd, NY)
                     + part_of(jnp.broadcast_to(both[2:3], shape), zd, NZ)
                     + jnp.broadcast_to(quarter[0:1], shape))
        px = jnp.broadcast_to(both[0:1], shape)

        for x in range(cells):
            xd = (mx * cells + x - source_ref[0]).astype(jnp.float32)
            frac = base_frac + part_of(px, jnp.full(shape, xd), nx_total)
            frac = frac - jnp.floor(frac + 0.5)
            u = (2.0 * math.pi) * (0.25 - jnp.abs(frac))
            w = u * u
            p = -1.0 / 39916800.0 + w * (1.0 / 6227020800.0)
            for coef in (1.0 / 362880.0, -1.0 / 5040.0, 1.0 / 120.0, -1.0 / 6.0, 1.0):
                p = coef + w * p
            table[x] = u * p

    def halo_copy(s, side, part):
        peer = (left, right)[side]
        return remote(hs.at[s % 2, side, part], hr.at[s % 2, side, part], hss_sem.at[s, side, part],
                      hsr_sem.at[s, side, part], "xyz", peer)

    def put_halo(s, part, t, w, value):
        base = (t * share + w) * 6
        for c in range(6):
            hs[s % 2, 0, part, pl.ds(base + c, 1)] = value[c, 0:1]
            hs[s % 2, 1, part, pl.ds(base + c, 1)] = value[c, 7:8]

    def start_halos(s, part):
        for side in range(2):
            halo_copy(s, side, part).start()

    def receive(part):
        own_copy(part).wait()
        for d in range(1, n):
            field_copy(0, lax.rem(me + d, n), part).wait_recv()

        def first_halo(i, inner):
            t, w = i // share, i % share
            put_halo(0, part, t, w, lam[t, part * share + w])
            return inner

        lax.fori_loop(0, n * share, first_halo, 0)
        start_halos(0, part)

    def row_copy(d):
        return remote(rs.at[d], rr.at[d], rs_sem.at[d], rr_sem.at[d], "xyz", right)

    def take_links(d):
        for other in range(1, n):
            link_copy(d, 0, lax.rem(me + other, n)).wait_recv()

        @pl.when(d < distinct - 1)
        def _():
            def send_rows(t, carry):
                rs[d, t, 0:18] = lk[d, t, 18:36, 7, :]
                return carry

            lax.fori_loop(0, n, send_rows, 0)
            row_copy(d).start()

    def prepare(s, at, arrived):
        def pick(read):
            if distinct == SECTIONS:
                return read(s)
            value = read(0)
            for d in range(1, arrived):
                value = jnp.where(at == d, read(d), value)
            return value

        def backward(t, d, block):
            block = block.reshape(3, 3, 2, 8, 128)
            for a in range(3):
                re, im = block[:, a, 0], block[:, a, 1]
                cur[t, 3 + d, a * 9:(a + 1) * 9] = jnp.stack([re, re - im, -(re + im)], axis=1).reshape(9, 8, 128)

        def at_time(t, carry):
            for g in range(4):
                block = pick(lambda d: lk[d, t, g * 18:(g + 1) * 18])
                pair = block.reshape(9, 2, 8, 128)
                re, im = pair[:, 0], pair[:, 1]
                cur[t, g] = jnp.stack([re, re + im, im - re], axis=1).reshape(27, 8, 128)
                if g == 1:
                    backward(t, 1, roll3(block, 1, 1))
                if g == 2:
                    backward(t, 2, roll3(block, NZ, 2))
                if g == 3:
                    backward(t, 3, jnp.where((zc == 0)[None], roll3(block, 1 - NZ, 2), roll3(block, 1, 2)))
            return carry

        lax.fori_loop(0, n, at_time, 0)

        @pl.when(s < distinct - 1)
        def _():
            row_copy(s).wait_recv()

        @pl.when(s == distinct - 1)
        def _():
            for other in range(1, n):
                last_rows_copy(0, lax.rem(me + other, n)).wait_recv()

        def edge_rows(t, carry):
            rows = pick(lambda d: rr[d, t, 0:18]).reshape(3, 3, 2, 128)
            for a in range(3):
                re, im = rows[:, a, 0], rows[:, a, 1]
                new = jnp.stack([re, re - im, -(re + im)], axis=1).reshape(9, 1, 128)
                old = cur[t, 4, a * 9:(a + 1) * 9]
                cur[t, 4, a * 9:(a + 1) * 9] = jnp.where((sub == 0)[None], jnp.broadcast_to(new, (9, 8, 128)), old)
            return carry

        lax.fori_loop(0, n, edge_rows, 0)

    def lap(s, part, source, epilogue, after_time):
        par = s % 2

        def at_time(i, carry):
            t = jnp.where(me < n // 2, n - 1 - i, i)
            prev, following = lax.rem(t + n - 1, n), lax.rem(t + 1, n)

            def links(time, d):
                return cur[time, d].reshape(3, 3, 3, 8, 128)

            def at_spinors(g, inner):
                qs, rows, vs = [], [], []
                for e in range(group):
                    w = g * group + e
                    qs.append(part * share + w)
                    rows.append((t * share + w) * 6)
                    vs.append(source[t, qs[e]])
                accs = [(None, None, None)] * group

                def step(link, xs, conj):
                    for e in range(group):
                        accs[e] = hop(accs[e], link, xs[e], conj)

                def edge(side, e):
                    return jnp.stack([jnp.broadcast_to(hr[par, side, part, pl.ds(rows[e] + c, 1)], (8, 128))
                                      for c in range(6)])

                step(links(t, 0), [source[following, q] for q in qs], False)
                step(links(prev, 0), [source[prev, q] for q in qs], True)
                step(links(t, 1), [jnp.where((sub == 7)[None], edge(0, e), roll3(vs[e], -1, 1))
                                   for e in range(group)], False)
                step(links(t, 4), [jnp.where((sub == 0)[None], edge(1, e), roll3(vs[e], 1, 1))
                                   for e in range(group)], False)
                step(links(t, 2), [roll3(v, -NZ, 2) for v in vs], False)
                step(links(t, 5), [roll3(v, NZ, 2) for v in vs], False)
                step(links(t, 3), [jnp.where((zc == NZ - 1)[None], roll3(v, NZ - 1, 2), roll3(v, -1, 2))
                                   for v in vs], False)
                step(links(t, 6), [jnp.where((zc == 0)[None], roll3(v, 1 - NZ, 2), roll3(v, 1, 2))
                                   for v in vs], False)
                for e in range(group):
                    acc = accs[e]
                    total = jnp.stack([acc[0] - acc[1], acc[0] + acc[2]], axis=1).reshape(6, 8, 128)
                    nxt = epilogue(t, qs[e], total - 8.0 * vs[e], vs[e])
                    put_halo(s + 1, part, t, g * group + e, nxt)
                return inner

            lax.fori_loop(0, share // group, at_spinors, 0)
            after_time(t, part)
            return carry

        lax.fori_loop(0, n, at_time, 0)

    def ep_later(t, q, value, v):
        value = (0.75 * flow_step) * value
        later[t, q] = value
        return value

    def ep_middle(t, q, value, v):
        middle = lam[t, q] + (8.0 * flow_step / 9.0) * value
        lam[t, q] = middle + v
        value = (0.25 * flow_step) * middle - (2.0 * flow_step / 9.0) * v
        mixed[t, q] = value
        return value

    def ep_last(t, q, value, v):
        value = lam[t, q] + value
        lam[t, q] = value
        square = value * value
        square = (square[0] + square[1]) + (square[2] + square[3]) + (square[4] + square[5])
        sign = jnp.where(lax.rem(q, 4) < 2, 1.0, -1.0)
        dens[t] = dens[t] + sign * square
        return value

    def out_copy(t, part, j):
        return remote(lam.at[t, pl.ds(part * share, share)],
                      out_ref.at[pl.ds(j * nc + part * share, share)],
                      os_sem.at[t, part], or_sem.at[j, part], "ta", t)

    def nothing(t, part):
        return None

    def step_body(i, carry):
        for k, (source, epilogue) in enumerate(((lam, ep_later), (later, ep_middle), (mixed, ep_last))):
            s = i * 3 + k

            def give(t, part):
                @pl.when(jnp.logical_and(s + 1 == SECTIONS, t != me))
                def _():
                    out_copy(t, part, mine).start()

            @pl.when(s == distinct - 1)
            def _():
                take_links(s)

            for step in range(STEPS):
                @pl.when(i == step)
                def _():
                    prepare(s, place[step * 3 + k], min(distinct, step * 3 + k + 1))

            if k == 0:
                @pl.when(s == 0)
                def _():
                    receive(0)

            if k == 2:
                dens[...] = jnp.zeros(dens.shape, jnp.float32)

            def at_part(part, inner):
                if k == 0:
                    @pl.when(jnp.logical_and(s == 0, part + 1 < parts))
                    def _():
                        receive(part + 1)

                @pl.when(jnp.logical_and(part == parts - 1, s + 1 < distinct - 1))
                def _():
                    take_links(s + 1)

                for side in range(2):
                    halo_copy(s, side, part).wait()
                lap(s, part, source, epilogue, give if k == 2 else nothing)

                @pl.when(s + 1 < SECTIONS)
                def _():
                    start_halos(s + 1, part)

                @pl.when(s + 1 == SECTIONS)
                def _():
                    mine_at = mine * nc + part * share
                    out_ref[pl.ds(mine_at, share)] = lam[me, pl.ds(part * share, share)]
                return inner

            lax.fori_loop(0, parts, at_part, 0)
        return carry

    def x_copy(d):
        return remote(pjs, pjr.at[mx], xs_sem.at[d - 1], xr_sem.at[mx], "xyz", lax.rem(mx + d, nx))

    def x_arrival(j):
        return remote(pjs, pjr.at[j], xs_sem.at[0], xr_sem.at[j], "xyz", j)

    def t_copy(t):
        return remote(pjt.at[t], pjf.at[mine], ts_sem.at[t], tr_sem.at[mine], "ta", t)

    @pl.when(worker)
    def _():
        fill_table()
        take_links(0)
        lax.fori_loop(0, STEPS, step_body, 0)
        rows = dens[...].reshape(n * 8, 128)
        cell = lax.broadcasted_iota(jnp.int32, (n * 8, 128), 0) % 8
        acc = jnp.zeros((n * 8, 128), jnp.float32)
        for x in range(cells):
            product = jnp.dot(rows, table[x], precision=lax.Precision.HIGHEST, preferred_element_type=jnp.float32)
            acc = acc + jnp.where(cell == x, product, 0.0)
        pjs[...] = jnp.broadcast_to(jnp.sum(acc.reshape(n, 8, 128), axis=1, keepdims=True), (n, 8, 128))
        pjr[mx] = pjs[...]
        for d in range(1, nx):
            x_copy(d).start()
        for d in range(1, nx):
            x_arrival(lax.rem(mx + d, nx)).wait_recv()
        total = pjr[0]
        for j in range(1, nx):
            total = total + pjr[j]
        pjt[...] = total
        pjf[mine] = pjt[me]
        for d in range(1, n):
            t_copy(lax.rem(me + d, n)).start()

    for j in range(workers):
        @pl.when(me != lo + j)
        def _():
            remote(pjt.at[0], pjf.at[j], ts_sem.at[0], tr_sem.at[j], "ta", lo + j).wait_recv()
    final = pjf[0]
    for j in range(1, workers):
        final = final + pjf[j]
    final = final * (1.0 / math.sqrt(576.0 * cells * nx * NY * NZ))
    proj_ref[0] = final[0:1, 0:nmom]
    proj_ref[1] = pltpu.roll(final, 64, 1)[0:1, 0:nmom]

    def drain(act):
        to_workers(act)

    def drain_parts(part, carry):
        to_workers(lambda j: field_copy(j, me, part).wait_send())
        return carry

    def drain_links(s, carry):
        to_workers(lambda j: link_copy(s, j, me).wait_send())
        return carry

    lax.fori_loop(0, parts, drain_parts, 0)
    lax.fori_loop(0, distinct, drain_links, 0)
    edge_copy().wait_send()
    to_workers(lambda j: last_rows_copy(j, me).wait_send())

    @pl.when(worker)
    def _():
        def drain_rows(s, carry):
            row_copy(s).wait_send()
            return carry

        lax.fori_loop(0, distinct - 1, drain_rows, 0)
        for d in range(1, nx):
            x_copy(d).wait_send()
        for d in range(1, n):
            t_copy(lax.rem(me + d, n)).wait_send()

        def drain_out(part, carry):
            for d in range(1, n):
                out_copy(lax.rem(me + d, n), part, mine).wait_send()
            return carry

        lax.fori_loop(0, parts, drain_out, 0)

    def arrivals(part, carry):
        for j in range(workers):
            @pl.when(me != lo + j)
            def _():
                out_copy(lo + j, part, j).wait_recv()
        return carry

    lax.fori_loop(0, parts, arrivals, 0)


def flow(n, nx, distinct, sink, links, section_index, momenta, source):
    space_cells = sink.shape[5]
    spinors = sink.shape[0] * sink.shape[1]
    slots = links.shape[0]
    nmom = momenta.shape[0]
    lo = n // 4 if spinors % (n - 2 * (n // 4)) == 0 else 0
    hi = n - lo
    nc = spinors // (hi - lo)
    parts = next(p for p in (4, 3, 2, 1) if nc % p == 0)
    share = nc // parts
    workers = hi - lo
    tile = (space_cells, NY * NZ)
    f32 = jnp.float32
    field = pltpu.VMEM((n, nc, 6) + tile, f32)
    halo = pltpu.VMEM((2, 2, parts, n * share * 6, NY * NZ), f32)
    dma = pltpu.SemaphoreType.DMA
    anywhere = pl.BlockSpec(memory_space=pl.ANY)
    vmem = pl.BlockSpec(memory_space=pltpu.VMEM)
    smem = pl.BlockSpec(memory_space=pltpu.SMEM)
    out, proj = pl.pallas_call(
        functools.partial(kernel, n, nx, nc, lo, hi, parts, nmom, distinct),
        out_shape=(
            pltpu.VMEM((spinors, 6) + tile, f32),
            pltpu.VMEM((2, 1, nmom), f32),
        ),
        in_specs=[smem, smem, vmem, anywhere, anywhere],
        out_specs=(vmem, vmem),
        scratch_shapes=[
            pltpu.VMEM((slots, 72) + tile, f32),
            pltpu.VMEM((distinct, n, 72) + tile, f32),
            pltpu.VMEM((n, 7, 27) + tile, f32),
            field, field, field,
            halo, halo,
            pltpu.VMEM((distinct, n, 24, NY * NZ), f32),
            pltpu.VMEM((distinct, n, 24, NY * NZ), f32),
            pltpu.VMEM((24, NY * NZ), f32),
            pltpu.VMEM((24, NY * NZ), f32),
            pltpu.VMEM((space_cells, NY * NZ, 128), f32),
            pltpu.VMEM((n,) + tile, f32),
            pltpu.VMEM((n, 8, 128), f32),
            pltpu.VMEM((nx, n, 8, 128), f32),
            pltpu.VMEM((n, 8, 128), f32),
            pltpu.VMEM((workers, 8, 128), f32),
            dma((slots,)), dma((parts,)),
            dma((workers, parts)), dma((n, parts)),
            dma((distinct, workers)), dma((distinct, n)),
            dma((SECTIONS, 2, parts)), dma((SECTIONS, 2, parts)),
            dma((distinct,)), dma((distinct,)),
            dma((1,)), dma((1,)), dma((workers,)), dma((n,)),
            dma((n, parts)), dma((workers, parts)),
            dma((nx - 1,)), dma((nx,)),
            dma((n,)), dma((workers,)),
        ],
        compiler_params=pltpu.CompilerParams(
            collective_id=distinct, has_side_effects=True, vmem_limit_bytes=60 * 1024 * 1024
        ),
    )(section_index, source, momenta.T, sink.reshape((spinors, 6) + tile), links.reshape((slots, 72) + tile))
    return (out, proj)


def count_slots(order_ref, choice_ref):
    named = [order_ref[s // 3, s % 3] for s in range(SECTIONS)]
    count = jnp.int32(1)
    for s in range(1, SECTIONS):
        fresh = functools.reduce(jnp.logical_and, [named[s] != named[j] for j in range(s)])
        count = count + fresh.astype(jnp.int32)
    choice_ref[0] = jnp.maximum(count - FEWEST, 0)


def body(n, nx, sink, links, section_index, momenta, source):
    smem = pl.BlockSpec(memory_space=pltpu.SMEM)
    choice = pl.pallas_call(count_slots, out_shape=jax.ShapeDtypeStruct((1,), jnp.int32),
                            in_specs=[smem], out_specs=smem)(section_index)
    branches = [functools.partial(flow, n, nx, distinct) for distinct in range(FEWEST, SECTIONS + 1)]
    out, proj = lax.switch(choice[0], branches, sink, links, section_index, momenta, source)
    return (out.reshape(sink.shape), jnp.transpose(proj, (0, 2, 1)))


def solution(mesh):
    in_specs = (
        P("cfg", None, None, None, "ta", "xyz", None),
        P("cfg", None, None, None, None, "ta", "xyz", None),
        P(),
        P(),
        P(),
    )
    out_specs = (P("cfg", None, None, None, "ta", "xyz", None), P("cfg", None, "ta"))
    step = functools.partial(body, mesh.shape["ta"], mesh.shape["xyz"])
    return jax.shard_map(step, mesh=mesh, in_specs=in_specs, out_specs=out_specs, check_vma=False)
```

```python
import functools
import math

import jax
import jax.numpy as jnp
from jax import lax
from jax.experimental import pallas as pl
from jax.experimental.pallas import tpu as pltpu
from jax.sharding import PartitionSpec as P

STEPS = 2
NY = 16
NZ = 8
SECTIONS = 3 * STEPS
GROUP = 2
PARTS = (6, 4, 3, 2, 1)
MESH = pl.DeviceIdType.MESH

flow_step = 0.05


def remote(src, dst, send_sem, recv_sem, axis, peer):
    return pltpu.make_async_remote_copy(
        src_ref=src, dst_ref=dst, send_sem=send_sem, recv_sem=recv_sem,
        device_id={axis: peer}, device_id_type=MESH,
    )


def roll3(x, amount, axis):
    shape = x.shape
    flat = x.reshape((-1,) + shape[-2:])
    return pltpu.roll(flat, amount % flat.shape[axis], axis).reshape(shape)


def hop(acc, link, x, conj):
    one, two, three = acc
    for k in range(3):
        vr, vi = x[2 * k], x[2 * k + 1]
        vs = (vr + vi)[None]
        if conj:
            block = link[k]
            a, b, c = block[:, 0] * vs, block[:, 2] * vi[None], block[:, 1] * vr[None]
            two = -b if two is None else two - b
            three = -c if three is None else three - c
        else:
            block = link[:, k]
            a, b, c = block[:, 0] * vs, block[:, 1] * vi[None], block[:, 2] * vr[None]
            two = b if two is None else two + b
            three = c if three is None else three + c
        one = a if one is None else one + a
    return one, two, three


COEFS = (0.75 * flow_step, 8.0 * flow_step / 9.0, 1.0)


def kernel(n, nx, nc, lo, hi, parts, batches, keep, nmom, distinct, last_at, order_ref, source_ref, momenta_ref, sink_ref, link_ref,
           out_ref, proj_ref,
           raw, lk, cur, lam, later, mixed, hs, hr, rs, rr, edge_out, edge_in, table, dens, pjs, pjr, pjt, pjf,
           raw_sem, loc_sem, fs_sem, fr_sem, ls_sem, lr_sem,
           hss_sem, hsr_sem, rs_sem, rr_sem, es_sem, er_sem, gs_sem, gr_sem, os_sem, or_sem,
           xs_sem, xr_sem, ts_sem, tr_sem):
    me = lax.axis_index("ta")
    mx = lax.axis_index("xyz")
    worker = jnp.logical_and(me >= lo, me < hi)
    mine = me - lo
    workers = hi - lo
    share = nc // parts
    group = GROUP if share % GROUP == 0 else 1
    slots = raw.shape[0]
    cells = 8
    left, right = lax.rem(mx + nx - 1, nx), lax.rem(mx + 1, nx)
    sub = lax.broadcasted_iota(jnp.int32, (8, 128), 0)
    zc = lax.broadcasted_iota(jnp.int32, (8, 128), 1) % NZ
    lane_at = lax.broadcasted_iota(jnp.int32, (8, 128), 1)
    up = jnp.where(zc == NZ - 1, lane_at - (NZ - 1), lane_at + 1)
    down = jnp.where(zc == 0, lane_at + (NZ - 1), lane_at - 1)

    def lanes(x, at):
        return jnp.stack([jnp.take_along_axis(x[c], at, axis=1, mode="promise_in_bounds") for c in range(6)])


    for slot in range(slots):
        pltpu.make_async_copy(link_ref.at[slot], raw.at[slot], raw_sem.at[slot]).start()

    def own_copy(part):
        return pltpu.make_async_copy(sink_ref.at[pl.ds(mine * nc + part * share, share)],
                                     lam.at[me, pl.ds(part * share, share)], loc_sem.at[part])

    @pl.when(worker)
    def _():
        for part in range(parts):
            own_copy(part).start()

    named = [order_ref[STEPS - 1 - s // 3, 2 - s % 3] for s in range(SECTIONS)]
    first, place = [], []
    count = jnp.int32(0)
    for s in range(SECTIONS):
        at = count
        for j in reversed(range(s)):
            at = jnp.where(named[j] == named[s], place[j], at)
        fresh = at == count
        first.append(fresh)
        place.append(at)
        count = count + fresh.astype(jnp.int32)
    held = []
    for d in range(distinct):
        slot = jnp.int32(0)
        for s in range(SECTIONS):
            slot = jnp.where(jnp.logical_and(first[s], place[s] == d), named[s], slot)
        held.append(slot)

    barrier = pltpu.get_barrier_semaphore()
    for d in range(1, n):
        pl.semaphore_signal(barrier, inc=1, device_id={"ta": lax.rem(me + d, n)}, device_id_type=MESH)
    for d in range(1, nx):
        pl.semaphore_signal(barrier, inc=1, device_id={"xyz": lax.rem(mx + d, nx)}, device_id_type=MESH)

    for slot in range(slots):
        pltpu.make_async_copy(link_ref.at[slot], raw.at[slot], raw_sem.at[slot]).wait()
    for d in range(distinct):
        for g in range(4):
            lk[d, me, g * 18:(g + 1) * 18] = raw[held[d], g * 18:(g + 1) * 18]
    edge_out[0:18] = raw[held[distinct - 1], 18:36, 7, :]

    pl.semaphore_wait(barrier, n + nx - 2)

    def field_copy(j, source, part):
        return remote(sink_ref.at[pl.ds(j * nc + part * share, share)],
                      lam.at[source, pl.ds(part * share, share)],
                      fs_sem.at[j, part], fr_sem.at[source, part], "ta", lo + j)

    def link_copy(d, j, source):
        return remote(lk.at[d, source], lk.at[d, source], ls_sem.at[d, j], lr_sem.at[d, source], "ta", lo + j)

    def edge_copy():
        return remote(edge_out, edge_in, es_sem.at[0], er_sem.at[0], "xyz", right)

    def last_rows_copy(j, source):
        return remote(edge_in, rr.at[distinct - 1, source], gs_sem.at[j], gr_sem.at[source], "ta", lo + j)

    def peer_order(i):
        return jnp.where(me < n // 2, workers - 1 - i, i)

    def to_workers(act):
        for i in range(workers):
            j = peer_order(i)

            @pl.when(me != lo + j)
            def _():
                act(j)

    edge_copy().start()
    to_workers(lambda j: link_copy(0, j, me).start())
    for part in range(parts):
        to_workers(lambda j: field_copy(j, me, part).start())
    for d in range(1, distinct - 1):
        to_workers(lambda j: link_copy(d, j, me).start())
    edge_copy().wait_recv()
    to_workers(lambda j: last_rows_copy(j, me).start())
    if distinct > 1:
        to_workers(lambda j: link_copy(distinct - 1, j, me).start())

    @pl.when(worker)
    def _():
        rr[distinct - 1, me] = edge_in[...]

    def fill_table():
        nx_total = cells * nx
        lane = lax.broadcasted_iota(jnp.int32, (8, 128), 1)
        table[0, 0:8] = jnp.zeros((8, 128), jnp.float32)
        table[0, 0:3, 0:nmom] = momenta_ref[...].astype(jnp.float32)
        base = table[0, 0:8]
        both = jnp.where(lane < 64, base, pltpu.roll(base, 64, 1))
        quarter = jnp.where(lane < 64, 0.0, 0.25)
        shape = (NY * NZ, 128)
        site = lax.broadcasted_iota(jnp.int32, shape, 0)
        yd = (site // NZ - source_ref[1]).astype(jnp.float32)
        zd = (site % NZ - source_ref[2]).astype(jnp.float32)

        def part_of(p, d, size):
            f = (p * d) * (1.0 / size)
            return f - jnp.floor(f)

        base_frac = (part_of(jnp.broadcast_to(both[1:2], shape), yd, NY)
                     + part_of(jnp.broadcast_to(both[2:3], shape), zd, NZ)
                     + jnp.broadcast_to(quarter[0:1], shape))
        px = jnp.broadcast_to(both[0:1], shape)

        for x in range(cells):
            xd = (mx * cells + x - source_ref[0]).astype(jnp.float32)
            frac = base_frac + part_of(px, jnp.full(shape, xd), nx_total)
            frac = frac - jnp.floor(frac + 0.5)
            u = (2.0 * math.pi) * (0.25 - jnp.abs(frac))
            w = u * u
            p = -1.0 / 39916800.0 + w * (1.0 / 6227020800.0)
            for coef in (1.0 / 362880.0, -1.0 / 5040.0, 1.0 / 120.0, -1.0 / 6.0, 1.0):
                p = coef + w * p
            table[x] = u * p

    def halo_copy(s, side, part):
        peer = (left, right)[side]
        return remote(hs.at[s % 2, side, part], hr.at[s % 2, side, part], hss_sem.at[s, side, part],
                      hsr_sem.at[s, side, part], "xyz", peer)

    def put_halo(s, part, t, w, value):
        base = (t * share + w) * 6
        for c in range(6):
            hs[s % 2, 0, part, pl.ds(base + c, 1)] = value[c, 0:1]
            hs[s % 2, 1, part, pl.ds(base + c, 1)] = value[c, 7:8]

    def start_halos(s, part):
        for side in range(2):
            halo_copy(s, side, part).start()

    def receive(part):
        own_copy(part).wait()
        for d in range(1, n):
            field_copy(0, lax.rem(me + d, n), part).wait_recv()

        def first_halo(i, inner):
            t, w = i // share, i % share
            put_halo(0, part, t, w, lam[t, part * share + w])
            return inner

        lax.fori_loop(0, n * share, first_halo, 0)
        start_halos(0, part)

    def row_copy(d):
        return remote(rs.at[d], rr.at[d], rs_sem.at[d], rr_sem.at[d], "xyz", right)

    def take_links(d):
        for other in range(1, n):
            link_copy(d, 0, lax.rem(me + other, n)).wait_recv()

        @pl.when(d < distinct - 1)
        def _():
            def send_rows(t, carry):
                rs[d, t, 0:18] = lk[d, t, 18:36, 7, :]
                return carry

            lax.fori_loop(0, n, send_rows, 0)
            row_copy(d).start()

    def cur_slot(s):
        return jnp.maximum(s - (distinct - 1), 0) if keep else 0

    def prepare(s, at, arrived, first_time):
        at_cur = cur_slot(s)
        turn_of = lax.rem(s, 3)
        coef = jnp.where(turn_of == 0, COEFS[0], jnp.where(turn_of == 1, COEFS[1], COEFS[2]))

        def pick(read):
            if distinct == SECTIONS:
                return read(s)
            value = read(0)
            for d in range(1, arrived):
                value = jnp.where(at == d, read(d), value)
            return value

        def backward(t, d, block):
            block = block.reshape(3, 3, 2, 8, 128)
            for a in range(3):
                re, im = block[:, a, 0], block[:, a, 1]
                cur[at_cur, t, 3 + d, a * 9:(a + 1) * 9] = jnp.stack([re, re - im, -(re + im)], axis=1).reshape(9, 8, 128)

        def at_time(t, carry):
            for g in range(4):
                block = coef * pick(lambda d: lk[d, t, g * 18:(g + 1) * 18])
                pair = block.reshape(9, 2, 8, 128)
                re, im = pair[:, 0], pair[:, 1]
                cur[at_cur, t, g] = jnp.stack([re, re + im, im - re], axis=1).reshape(27, 8, 128)
                if g == 1:
                    backward(t, 1, roll3(block, 1, 1))
                if g == 2:
                    backward(t, 2, roll3(block, NZ, 2))
                if g == 3:
                    backward(t, 3, jnp.where((zc == 0)[None], roll3(block, 1 - NZ, 2), roll3(block, 1, 2)))
            return carry

        lax.fori_loop(0, n, at_time, 0)

        @pl.when(s < distinct - 1)
        def _():
            row_copy(s).wait_recv()

        @pl.when(jnp.logical_and(s == last_at, first_time))
        def _():
            for other in range(1, n):
                last_rows_copy(0, lax.rem(me + other, n)).wait_recv()

        def edge_rows(t, carry):
            rows = (coef * pick(lambda d: rr[d, t, 0:18])).reshape(3, 3, 2, 128)
            for a in range(3):
                re, im = rows[:, a, 0], rows[:, a, 1]
                new = jnp.stack([re, re - im, -(re + im)], axis=1).reshape(9, 1, 128)
                old = cur[at_cur, t, 4, a * 9:(a + 1) * 9]
                cur[at_cur, t, 4, a * 9:(a + 1) * 9] = jnp.where((sub == 0)[None], jnp.broadcast_to(new, (9, 8, 128)), old)
            return carry

        lax.fori_loop(0, n, edge_rows, 0)

    def lap(s, part, source, epilogue, coef, after_time):
        par = s % 2
        at_cur = cur_slot(s)

        def at_time(i, carry):
            t = jnp.where(me < n // 2, n - 1 - i, i)
            prev, following = lax.rem(t + n - 1, n), lax.rem(t + 1, n)

            def links(time, d):
                return cur[at_cur, time, d].reshape(3, 3, 3, 8, 128)

            def at_spinors(g, inner):
                qs, rows, vs = [], [], []
                for e in range(group):
                    w = g * group + e
                    qs.append(part * share + w)
                    rows.append((t * share + w) * 6)
                    vs.append(source[t, qs[e]])
                accs = [(None, None, None)] * group

                def step(link, xs, conj):
                    for e in range(group):
                        accs[e] = hop(accs[e], link, xs[e], conj)

                def edge(side, e):
                    return jnp.stack([jnp.broadcast_to(hr[par, side, part, pl.ds(rows[e] + c, 1)], (8, 128))
                                      for c in range(6)])

                step(links(t, 0), [source[following, q] for q in qs], False)
                step(links(prev, 0), [source[prev, q] for q in qs], True)
                step(links(t, 1), [jnp.where((sub == 7)[None], edge(0, e), roll3(vs[e], -1, 1))
                                   for e in range(group)], False)
                step(links(t, 4), [jnp.where((sub == 0)[None], edge(1, e), roll3(vs[e], 1, 1))
                                   for e in range(group)], False)
                step(links(t, 2), [roll3(v, -NZ, 2) for v in vs], False)
                step(links(t, 5), [roll3(v, NZ, 2) for v in vs], False)
                step(links(t, 3), [lanes(v, up) for v in vs], False)
                step(links(t, 6), [lanes(v, down) for v in vs], False)
                for e in range(group):
                    acc = accs[e]
                    total = jnp.stack([acc[0] - acc[1], acc[0] + acc[2]], axis=1).reshape(6, 8, 128)
                    nxt = epilogue(s, t, qs[e], total - (8.0 * coef) * vs[e], vs[e])
                    put_halo(s + 1, part, t, g * group + e, nxt)
                return inner

            lax.fori_loop(0, share // group, at_spinors, 0)
            after_time(t, part)
            return carry

        lax.fori_loop(0, n, at_time, 0)

    def ep_later(s, t, q, value, v):
        later[t, q] = value
        return value

    def ep_middle(s, t, q, value, v):
        middle = lam[t, q] + value
        lam[t, q] = middle + v
        value = (0.25 * flow_step) * middle - (2.0 * flow_step / 9.0) * v
        mixed[t, q] = value
        return value

    def ep_last(s, t, q, value, v):
        value = lam[t, q] + value
        lam[t, q] = value
        square = value * value
        square = (square[0] + square[1]) + (square[2] + square[3]) + (square[4] + square[5])
        sign = jnp.where(s == SECTIONS - 1, jnp.where(lax.rem(q, 4) < 2, 1.0, -1.0), 0.0)
        dens[t] = dens[t] + sign * square
        return value

    def out_copy(t, part, j):
        return remote(lam.at[t, pl.ds(part * share, share)],
                      out_ref.at[pl.ds(j * nc + part * share, share)],
                      os_sem.at[t, part], or_sem.at[j, part], "ta", t)

    def nothing(t, part):
        return None

    tail = SECTIONS - (distinct - 1)
    batch = parts // batches

    def run(r, carry):
        late = r - (distinct - 1)
        whole = late < 0
        turn = jnp.where(whole, 0, late // tail)
        s = jnp.where(whole, r, distinct - 1 + late - turn * tail)
        begin = turn * batch
        end = jnp.where(whole, parts, begin + batch)

        @pl.when(jnp.logical_and(turn == 0, s == last_at))
        def _():
            take_links(distinct - 1)

        def get_ready(first_time):
            if distinct == SECTIONS:
                prepare(s, None, distinct, first_time)
                return
            for early in range(last_at):
                @pl.when(s == early)
                def _():
                    prepare(s, place[early], min(early + 1, distinct - 1), first_time)

            @pl.when(s >= last_at)
            def _():
                at = place[last_at]
                for other in range(last_at + 1, SECTIONS):
                    at = jnp.where(s == other, place[other], at)
                prepare(s, at, distinct, first_time)

        if keep:
            @pl.when(turn == 0)
            def _():
                get_ready(True)
        else:
            get_ready(turn == 0)

        @pl.when(r == 0)
        def _():
            receive(0)

        for k, (source, epilogue) in enumerate(((lam, ep_later), (later, ep_middle), (mixed, ep_last))):
            def give(t, part):
                @pl.when(jnp.logical_and(s + 1 == SECTIONS, t != me))
                def _():
                    out_copy(t, part, mine).start()

            def at_part(part, inner):
                if k == 0:
                    @pl.when(jnp.logical_and(s == 0, part + 1 < parts))
                    def _():
                        receive(part + 1)

                @pl.when(jnp.logical_and(part == parts - 1, s + 1 < distinct - 1))
                def _():
                    take_links(s + 1)

                for side in range(2):
                    halo_copy(s, side, part).wait()
                lap(s, part, source, epilogue, COEFS[k], give if k == 2 else nothing)

                @pl.when(s + 1 < SECTIONS)
                def _():
                    start_halos(s + 1, part)

                if k == 2:
                    @pl.when(s + 1 == SECTIONS)
                    def _():
                        mine_at = mine * nc + part * share
                        out_ref[pl.ds(mine_at, share)] = lam[me, pl.ds(part * share, share)]
                return inner

            @pl.when(lax.rem(s, 3) == k)
            def _():
                lax.fori_loop(begin, end, at_part, 0)
        return carry

    def x_copy(d):
        return remote(pjs, pjr.at[mx], xs_sem.at[d - 1], xr_sem.at[mx], "xyz", lax.rem(mx + d, nx))

    def x_arrival(j):
        return remote(pjs, pjr.at[j], xs_sem.at[0], xr_sem.at[j], "xyz", j)

    def t_copy(t):
        return remote(pjt.at[t], pjf.at[mine], ts_sem.at[t], tr_sem.at[mine], "ta", t)

    @pl.when(worker)
    def _():
        fill_table()
        take_links(0)
        dens[...] = jnp.zeros(dens.shape, jnp.float32)
        lax.fori_loop(0, distinct - 1 + batches * tail, run, 0)
        rows = dens[...].reshape(n * 8, 128)
        cell = lax.broadcasted_iota(jnp.int32, (n * 8, 128), 0) % 8
        acc = jnp.zeros((n * 8, 128), jnp.float32)
        for x in range(cells):
            product = jnp.dot(rows, table[x], precision=lax.Precision.HIGHEST, preferred_element_type=jnp.float32)
            acc = acc + jnp.where(cell == x, product, 0.0)
        pjs[...] = jnp.broadcast_to(jnp.sum(acc.reshape(n, 8, 128), axis=1, keepdims=True), (n, 8, 128))
        pjr[mx] = pjs[...]
        for d in range(1, nx):
            x_copy(d).start()
        for d in range(1, nx):
            x_arrival(lax.rem(mx + d, nx)).wait_recv()
        total = pjr[0]
        for j in range(1, nx):
            total = total + pjr[j]
        pjt[...] = total
        pjf[mine] = pjt[me]
        for d in range(1, n):
            t_copy(lax.rem(me + d, n)).start()

    for j in range(workers):
        @pl.when(me != lo + j)
        def _():
            remote(pjt.at[0], pjf.at[j], ts_sem.at[0], tr_sem.at[j], "ta", lo + j).wait_recv()
    final = pjf[0]
    for j in range(1, workers):
        final = final + pjf[j]
    final = final * (1.0 / math.sqrt(576.0 * cells * nx * NY * NZ))
    proj_ref[0] = final[0:1, 0:nmom]
    proj_ref[1] = pltpu.roll(final, 64, 1)[0:1, 0:nmom]

    def drain(act):
        to_workers(act)

    def drain_parts(part, carry):
        to_workers(lambda j: field_copy(j, me, part).wait_send())
        return carry

    def drain_links(s, carry):
        to_workers(lambda j: link_copy(s, j, me).wait_send())
        return carry

    lax.fori_loop(0, parts, drain_parts, 0)
    lax.fori_loop(0, distinct, drain_links, 0)
    edge_copy().wait_send()
    to_workers(lambda j: last_rows_copy(j, me).wait_send())

    @pl.when(worker)
    def _():
        def drain_rows(s, carry):
            row_copy(s).wait_send()
            return carry

        lax.fori_loop(0, distinct - 1, drain_rows, 0)
        for d in range(1, nx):
            x_copy(d).wait_send()
        for d in range(1, n):
            t_copy(lax.rem(me + d, n)).wait_send()

        def drain_out(part, carry):
            for d in range(1, n):
                out_copy(lax.rem(me + d, n), part, mine).wait_send()
            return carry

        lax.fori_loop(0, parts, drain_out, 0)

    def arrivals(part, carry):
        for j in range(workers):
            @pl.when(me != lo + j)
            def _():
                out_copy(lo + j, part, j).wait_recv()
        return carry

    lax.fori_loop(0, parts, arrivals, 0)


def flow(n, nx, distinct, last_at, sink, links, section_index, momenta, source):
    space_cells = sink.shape[5]
    spinors = sink.shape[0] * sink.shape[1]
    slots = links.shape[0]
    nmom = momenta.shape[0]
    lo = n // 4 if spinors % (n - 2 * (n // 4)) == 0 else 0
    hi = n - lo
    nc = spinors // (hi - lo)
    parts = next(p for p in PARTS if nc % p == 0)
    batches = 2 if parts % 2 == 0 else 1
    share = nc // parts
    workers = hi - lo
    tile = (space_cells, NY * NZ)
    f32 = jnp.float32
    field = pltpu.VMEM((n, nc, 6) + tile, f32)
    kept = SECTIONS - (distinct - 1)
    keep = kept * n * 7 * 27 * space_cells * NY * NZ * 4 < 16 * 1024 * 1024
    halo = pltpu.VMEM((2, 2, parts, n * share * 6, NY * NZ), f32)
    dma = pltpu.SemaphoreType.DMA
    anywhere = pl.BlockSpec(memory_space=pl.ANY)
    vmem = pl.BlockSpec(memory_space=pltpu.VMEM)
    smem = pl.BlockSpec(memory_space=pltpu.SMEM)
    out, proj = pl.pallas_call(
        functools.partial(kernel, n, nx, nc, lo, hi, parts, batches, keep, nmom, distinct, last_at),
        out_shape=(
            pltpu.VMEM((spinors, 6) + tile, f32),
            pltpu.VMEM((2, 1, nmom), f32),
        ),
        in_specs=[smem, smem, vmem, anywhere, anywhere],
        out_specs=(vmem, vmem),
        scratch_shapes=[
            pltpu.VMEM((slots, 72) + tile, f32),
            pltpu.VMEM((distinct, n, 72) + tile, f32),
            pltpu.VMEM((kept if keep else 1, n, 7, 27) + tile, f32),
            field, field, field,
            halo, halo,
            pltpu.VMEM((distinct, n, 24, NY * NZ), f32),
            pltpu.VMEM((distinct, n, 24, NY * NZ), f32),
            pltpu.VMEM((24, NY * NZ), f32),
            pltpu.VMEM((24, NY * NZ), f32),
            pltpu.VMEM((space_cells, NY * NZ, 128), f32),
            pltpu.VMEM((n,) + tile, f32),
            pltpu.VMEM((n, 8, 128), f32),
            pltpu.VMEM((nx, n, 8, 128), f32),
            pltpu.VMEM((n, 8, 128), f32),
            pltpu.VMEM((workers, 8, 128), f32),
            dma((slots,)), dma((parts,)),
            dma((workers, parts)), dma((n, parts)),
            dma((distinct, workers)), dma((distinct, n)),
            dma((SECTIONS, 2, parts)), dma((SECTIONS, 2, parts)),
            dma((distinct,)), dma((distinct,)),
            dma((1,)), dma((1,)), dma((workers,)), dma((n,)),
            dma((n, parts)), dma((workers, parts)),
            dma((nx - 1,)), dma((nx,)),
            dma((n,)), dma((workers,)),
        ],
        compiler_params=pltpu.CompilerParams(
            collective_id=PLANS.index((distinct, last_at)), has_side_effects=True, vmem_limit_bytes=60 * 1024 * 1024
        ),
    )(section_index, source, momenta.T, sink.reshape((spinors, 6) + tile), links.reshape((slots, 72) + tile))
    return (out, proj)


PLANS = ((3, 2), (3, 3), (4, 3), (4, 4), (5, 4), (5, 5), (6, 5))


def choose_plan(order_ref, choice_ref):
    named = [order_ref[STEPS - 1 - s // 3, 2 - s % 3] for s in range(SECTIONS)]
    count = jnp.int32(1)
    newest = jnp.int32(0)
    for s in range(1, SECTIONS):
        fresh = functools.reduce(jnp.logical_and, [named[s] != named[j] for j in range(s)])
        count = count + fresh.astype(jnp.int32)
        newest = jnp.where(fresh, s, newest)
    late = (newest > count - 1).astype(jnp.int32)
    choice_ref[0] = jnp.where(count < 3, 1, (count - 3) * 2 + late)


def body(n, nx, sink, links, section_index, momenta, source):
    smem = pl.BlockSpec(memory_space=pltpu.SMEM)
    choice = pl.pallas_call(choose_plan, out_shape=jax.ShapeDtypeStruct((1,), jnp.int32),
                            in_specs=[smem], out_specs=smem)(section_index)
    branches = [functools.partial(flow, n, nx, *plan) for plan in PLANS]
    out, proj = lax.switch(choice[0], branches, sink, links, section_index, momenta, source)
    return (out.reshape(sink.shape), jnp.transpose(proj, (0, 2, 1)))


def solution(mesh):
    in_specs = (
        P("cfg", None, None, None, "ta", "xyz", None),
        P("cfg", None, None, None, None, "ta", "xyz", None),
        P(),
        P(),
        P(),
    )
    out_specs = (P("cfg", None, None, None, "ta", "xyz", None), P("cfg", None, "ta"))
    step = functools.partial(body, mesh.shape["ta"], mesh.shape["xyz"])
    return jax.shard_map(step, mesh=mesh, in_specs=in_specs, out_specs=out_specs, check_vma=False)
```
